32 devices in a mesh: rep: 4 (over y, core), gx: 4 (over z), gy: 2 (over x).
Axes of the slice: x: 2, y: 2, z: 4, core: 2. Of those that a mesh axis runs over, the one named last changes fastest.
Arguments:
- hidden_one: bfloat16 [512, 8192], P(('rep', 'gy'), 'gx'), may hold values from -6 to 6
- hidden_two: bfloat16 [512, 8192], P(('rep', 'gy'), 'gx'), may hold values from -6 to 6
- w_qkv: bfloat16 [8192, 10240], P('gx', 'gy'), may hold values from -0.0625 to 0.0625
- w_out: bfloat16 [8192, 8192], P('gy', 'gx'), may hold values from -0.0625 to 0.0625
- key_cache: bfloat16 [512, 128, 1024], P(('rep', 'gx'), None, 'gy'), may hold values from -1000 to 1000
- value_cache: bfloat16 [512, 128, 1024], P(('rep', 'gx'), None, 'gy'), may hold values from -6 to 6
- lengths: int32 [4, 128], P(None, 'gx'), may hold values from 1 to 126, 8064 in all within a row
- mig_rows: int32 [4, 8, 2], P(None, 'gx'), may hold values from 0 to 15, as said below
- dest: int32 [4, 8, 2], P(None, 'gx'), may hold values from 0 to 3, as said below
Outputs:
- out_one: bfloat16 [512, 8192], P(('rep', 'gy'), 'gx')
- out_two: bfloat16 [512, 8192], P(('rep', 'gy'), 'gx')
The draws below stay inside these ranges and needn't reach their ends.
Inputs may be any that keep to these rules, and one draw needn't show every extreme that they name: mig_rows[r, p, :] are distinct; rows p * 16 + mig_rows[r, p, k] of replica r leave. For every block p and slot k, dest[:, p, k] names every replica once; the entries of dest[r, p, :] are distinct. The 128 lengths of each replica sum to 8064.
All inputs are finite; a program needn't handle non-finite values. No bound on the sum of `lengths` on one device may be relied on, other than what follows from the above.
Results may differ from the reference program's by a relative error of at most 0.015.
Values may be sent and summed in bfloat16 or wider, within the bound.
No kernel may reach another device: no remote copies, remote signals or barrier semaphores. Data moves between devices by JAX's collectives and lax.ppermute only.
A program may use at most 128 MiB of HBM per device.

```python
import math
import jax
import jax.numpy as jnp
import numpy as np
from jax import lax

D = 8192
HEADS = 64
KV_HEADS = 8
HEAD_DIM = 128
ROWS_DEV = 16
SLOTS = 128
MIG_DEV = 2
NREP = 4
NG = 8
ROWS = 128


def draw_mig_rows(key, part):
    seed_keys = jax.random.split(jax.random.fold_in(key, 11), NREP * NG)

    def pick_rows(seed_key):
        return jax.random.permutation(seed_key, ROWS_DEV)[:MIG_DEV]
    picked = jax.vmap(pick_rows)(seed_keys)
    return picked.reshape(NREP, NG, MIG_DEV).astype(jnp.int32)


def draw_dest(key, part):
    seed_keys = jax.random.split(jax.random.fold_in(key, 7), NG)

    def one_block(seed_key):
        first_key, second_key = jax.random.split(seed_key)
        ordering = jax.random.permutation(first_key, NREP)
        stride = jax.random.randint(second_key, (), 1, NREP)
        replica_ids = jnp.arange(NREP)
        columns = [ordering[(replica_ids + column * stride) % NREP] for column in range(MIG_DEV)]
        return jnp.stack(columns, axis=1)
    blocks = jax.vmap(one_block)(seed_keys)
    return jnp.transpose(blocks, (1, 0, 2)).astype(jnp.int32)


def draw_key_cache(key, part):
    row_total = NREP * ROWS
    row_width = KV_HEADS * HEAD_DIM
    return jnp.clip(jax.random.normal(jax.random.fold_in(key, 5), (row_total, SLOTS, row_width), jnp.float32), -6.0, 6.0).astype(jnp.bfloat16)


def block_scale(stream_key, shape, cuts, low, largest):
    gain = 1.0
    for position, parts in cuts:
        steps = jax.random.uniform(jax.random.fold_in(jax.random.fold_in(stream_key, 6), position), (parts,), jnp.float32, low / len(cuts), largest / len(cuts))
        gain = gain * jnp.repeat(jnp.exp(steps), shape[position] // parts).reshape((-1,) + (1,) * (len(shape) - 1 - position))
    return gain


def length_profile(amount, total, most, skew):
    loads = [(1 << 20) // math.isqrt(grade ** skew) + 1 for grade in range(2, amount + 1)]
    rest, holding = total - most - (amount - 1), [1] * (amount - 1)
    while rest > 0:
        candidates = [i for i in range(amount - 1) if holding[i] < most]
        whole, left = sum([loads[i] for i in candidates]), rest
        for i in candidates:
            more = min(most - holding[i], max(1, left * loads[i] // whole), rest)
            holding[i] = holding[i] + more
            rest = rest - more
    return np.array([most] + holding)


def ragged(rng, amount, total, reach, skew):
    if amount == 2:
        one = jax.random.randint(rng, (), max(1, total - reach), min(reach, total - 1) + 1)
        return jnp.stack([one, total - one])
    tallies = jnp.asarray(length_profile(amount, total, reach, skew), jnp.int32)
    twos = (amount - 1) // 2
    source_of, sink = tallies[1:1 + 2 * twos:2], tallies[2:2 + 2 * twos:2]
    margin = jnp.minimum(source_of - 1, reach - sink)
    shifted = jax.random.randint(jax.random.fold_in(rng, 1), (twos,), 0, 1 << 20) % (margin + 1)
    tallies = tallies.at[1:1 + 2 * twos:2].set(source_of - shifted).at[2:2 + 2 * twos:2].set(sink + shifted)
    return tallies[jax.random.permutation(jax.random.fold_in(rng, 2), amount)]


def gaussian(own_key, extent, width, limit, shards=(), kind=jnp.bfloat16):
    factor_of = block_scale(own_key, extent, shards, -0.22, 0.18) if shards else 1.0
    array = jax.random.normal(own_key, extent, jnp.float32) * width * factor_of
    return jnp.minimum(jnp.maximum(array, -limit), limit).astype(kind)


def setup_inputs(seed: int = 0) -> dict:
    key_of = jax.random.split(jax.random.key(seed), 10)
    return {
        "hidden_one": gaussian(key_of[0], (NREP * ROWS, D), 1.0, 6.0, ((0, 8), (1, 4))),
        "hidden_two": gaussian(key_of[1], (NREP * ROWS, D), 1.0, 6.0, ((0, 8), (1, 4))),
        "w_qkv": gaussian(key_of[2], (D, KV_HEADS * (HEADS // KV_HEADS + 2) * HEAD_DIM), D ** -0.5, 0.0625, ((0, 4), (1, 2))),
        "w_out": gaussian(key_of[3], (HEADS * HEAD_DIM, D), (HEADS * HEAD_DIM) ** -0.5, 0.0625, ((0, 2), (1, 4))),
        "key_cache": draw_key_cache(jax.random.fold_in(key_of[9], 71), 0),
        "value_cache": gaussian(key_of[5], (NREP * ROWS, SLOTS, KV_HEADS * HEAD_DIM), 1.0, 6.0, ((0, 16), (2, 2))),
        "lengths": jax.vmap(lambda own: ragged(own, ROWS, ROWS * (SLOTS - 2) // 2, SLOTS - 2, 2))(jax.random.split(key_of[6], NREP)).reshape((NREP, ROWS)).astype(jnp.int32),
        "mig_rows": draw_mig_rows(jax.random.fold_in(key_of[9], 71), 0),
        "dest": draw_dest(jax.random.fold_in(key_of[9], 71), 0),
    }


ROPE_BASE = 500000.0

def rotate(vectors, positions):
    half_dim = vectors.shape[-1] // 2
    inverse = ROPE_BASE ** (-(jnp.arange(half_dim, dtype=jnp.float32) * 2.0 / vectors.shape[-1]))
    angles = positions.astype(jnp.float32)[:, None, None] * inverse[None, None, :]
    cosine = jnp.cos(angles)
    sine_part = jnp.sin(angles)
    first_half = vectors[..., :half_dim]
    second_half = vectors[..., half_dim:]
    return jnp.concatenate([first_half * cosine - second_half * sine_part, second_half * cosine + first_half * sine_part], axis=-1)

def project(hidden, w_qkv, positions):
    row_count = hidden.shape[0]
    group_size = HEADS // KV_HEADS
    totals = jnp.dot(hidden, w_qkv, preferred_element_type=jnp.float32)
    totals = totals.reshape(row_count, KV_HEADS, group_size + 2, HEAD_DIM)
    queries = rotate(totals[:, :, :group_size].reshape(row_count, HEADS, HEAD_DIM), positions).astype(jnp.bfloat16)
    new_keys = rotate(totals[:, :, group_size], positions)
    new_keys = new_keys.reshape(row_count, KV_HEADS * HEAD_DIM).astype(jnp.bfloat16)
    new_values = totals[:, :, group_size + 1].reshape(row_count, KV_HEADS * HEAD_DIM).astype(jnp.bfloat16)
    return (queries, new_keys, new_values)

def attend(queries, cache_keys, cache_values, live_count, new_keys, new_values):
    row_count = queries.shape[0]
    slot_count = cache_keys.shape[1]
    group_size = HEADS // KV_HEADS
    score_scale = 1.0 / math.sqrt(HEAD_DIM)
    grouped = queries.reshape(row_count, KV_HEADS, group_size, HEAD_DIM).astype(jnp.float32)
    keys_split = cache_keys.reshape(row_count, slot_count, KV_HEADS, HEAD_DIM).astype(jnp.float32)
    values_split = cache_values.reshape(row_count, slot_count, KV_HEADS, HEAD_DIM).astype(jnp.float32)
    scores = jnp.einsum('ngjd,nsgd->ngjs', grouped, keys_split) * score_scale
    live_mask = (jnp.arange(slot_count, dtype=jnp.int32)[None, :] < live_count[:, None])[:, None, None, :]
    highest = lax.optimization_barrier(jnp.max(jnp.where(live_mask, scores, -jnp.inf), axis=-1))
    weights = jnp.where(live_mask, jnp.exp(scores - highest[..., None]), 0.0)
    weight_sum = lax.optimization_barrier(jnp.sum(weights, axis=-1))
    rounded = lax.optimization_barrier(weights.astype(jnp.bfloat16)).astype(jnp.float32)
    blended = jnp.einsum('ngjs,nsgd->ngjd', rounded, values_split)
    fresh_keys = new_keys.reshape(row_count, KV_HEADS, HEAD_DIM).astype(jnp.float32)
    fresh_score = jnp.einsum('ngjd,ngd->ngj', grouped, fresh_keys) * score_scale
    joint_max = jnp.maximum(highest, fresh_score)
    old_share = jnp.exp(highest - joint_max)
    new_share = jnp.exp(fresh_score - joint_max)
    fresh_values = new_values.reshape(row_count, KV_HEADS, 1, HEAD_DIM).astype(jnp.float32)
    merged = (old_share[..., None] * blended + new_share[..., None] * fresh_values) / (old_share * weight_sum + new_share)[..., None]
    return merged.reshape(row_count, HEADS * HEAD_DIM).astype(jnp.bfloat16)

def reference(hidden_one, hidden_two, w_qkv, w_out, key_cache, value_cache, lengths, mig_rows, dest):
    row_total = NREP * ROWS
    block_count = row_total // ROWS_DEV
    key_width = KV_HEADS * HEAD_DIM
    flat_lengths = lengths.reshape(row_total).astype(jnp.int32)
    query_one, key_one, value_one = project(hidden_one, w_qkv, flat_lengths)

    def first_block(pieces):
        queries, cache_keys, cache_values, live_count, new_keys, new_values = pieces
        return attend(queries, cache_keys, cache_values, live_count, new_keys, new_values)
    attended_one = lax.map(first_block, (query_one.reshape(block_count, ROWS_DEV, HEADS, HEAD_DIM), key_cache.reshape(block_count, ROWS_DEV, SLOTS, key_width), value_cache.reshape(block_count, ROWS_DEV, SLOTS, key_width), flat_lengths.reshape(block_count, ROWS_DEV), key_one.reshape(block_count, ROWS_DEV, key_width), value_one.reshape(block_count, ROWS_DEV, key_width))).reshape(row_total, HEADS * HEAD_DIM)
    out_one = jnp.dot(attended_one, w_out, preferred_element_type=jnp.float32).astype(jnp.bfloat16)
    replica_ids = jnp.arange(NREP, dtype=jnp.int32)[:, None, None]
    block_ids = jnp.arange(NG, dtype=jnp.int32)[None, :, None]
    landing = jnp.take_along_axis(mig_rows, dest, axis=0)
    target = (dest * ROWS + block_ids * ROWS_DEV + landing).reshape(-1).astype(jnp.int32)
    anchor = (replica_ids * ROWS + block_ids * ROWS_DEV + mig_rows).reshape(-1).astype(jnp.int32)
    source = jnp.arange(row_total, dtype=jnp.int32).at[target].set(anchor)
    live_two = flat_lengths[source] + 1
    query_two, key_two, value_two = project(hidden_two, w_qkv, live_two)
    slot_ids = jnp.arange(SLOTS, dtype=jnp.int32)

    def second_block(pieces):
        queries, rows_from, live_count, new_keys, new_values = pieces
        written = (slot_ids[None, :] == flat_lengths[rows_from][:, None])[:, :, None]
        cache_keys = jnp.where(written, key_one[rows_from][:, None, :], key_cache[rows_from])
        cache_values = jnp.where(written, value_one[rows_from][:, None, :], value_cache[rows_from])
        return attend(queries, cache_keys, cache_values, live_count, new_keys, new_values)
    attended_two = lax.map(second_block, (query_two.reshape(block_count, ROWS_DEV, HEADS, HEAD_DIM), source.reshape(block_count, ROWS_DEV), live_two.reshape(block_count, ROWS_DEV), key_two.reshape(block_count, ROWS_DEV, key_width), value_two.reshape(block_count, ROWS_DEV, key_width))).reshape(row_total, HEADS * HEAD_DIM)
    out_two = jnp.dot(attended_two, w_out, preferred_element_type=jnp.float32).astype(jnp.bfloat16)
    return (out_one, out_two)
```

```python
import math

import jax
import jax.numpy as jnp
from jax import lax
from jax.sharding import PartitionSpec as P

HEADS = 64
KV_HEADS = 8
HEAD_DIM = 128
ROWS_DEV = 16
GROUP = HEADS // KV_HEADS
ROPE_BASE = 500000.0
LINK_SCALE = 16.0
SCORE_SCALE = 1.0 / math.sqrt(HEAD_DIM)


def swap(value, axis, bit):
    count = lax.axis_size(axis)
    return lax.ppermute(value, axis, [(i, i ^ bit) for i in range(count)])


def power_of_two(count):
    return count & (count - 1) == 0


def gather_rows(hidden):
    if lax.axis_size("gy") != 2:
        return lax.all_gather(hidden, "gy", axis=0, tiled=True)
    peer = swap(hidden, "gy", 1)
    first = lax.axis_index("gy") == 0
    return jnp.concatenate([jnp.where(first, hidden, peer), jnp.where(first, peer, hidden)], axis=0)


def narrow(value):
    return (value * LINK_SCALE).astype(jnp.float16)


def widen(value):
    return value.astype(jnp.float32) * (1.0 / LINK_SCALE)


def project_sums(gathered, w_qkv):
    count = lax.axis_size("gx")
    if not power_of_two(count):
        return lax.psum_scatter(
            jnp.dot(gathered, w_qkv, preferred_element_type=jnp.float32),
            "gx", scatter_dimension=0, tiled=True,
        )
    place = lax.axis_index("gx")
    rows = gathered.shape[0] // count
    order = sorted(range(count), key=lambda k: [1 - (k >> b & 1) for b in range(count.bit_length() - 1)])
    blocks = [lax.dynamic_slice_in_dim(gathered, (place ^ k) * rows, rows, 0) for k in order]
    partial = jnp.dot(jnp.concatenate(blocks, axis=0), w_qkv, preferred_element_type=jnp.float32)
    bit = 1
    while bit < count:
        half = partial.shape[0] // 2
        received = swap(narrow(partial[:half]), "gx", bit)
        partial = partial[half:] + widen(received)
        bit *= 2
    return partial


def turn_tables(positions):
    half_dim = HEAD_DIM // 2
    inverse = ROPE_BASE ** (-(jnp.arange(half_dim, dtype=jnp.float32) * 2.0 / HEAD_DIM))
    angles = positions.astype(jnp.float32)[:, None] * inverse[None, :]
    return jnp.cos(angles), jnp.sin(angles)


def rotate(vectors, tables):
    half_dim = HEAD_DIM // 2
    cosine, sine = (t[:, None, None, :] for t in tables)
    first, second = vectors[..., :half_dim], vectors[..., half_dim:]
    return jnp.concatenate([first * cosine - second * sine, second * cosine + first * sine], axis=-1)


def split_sums(sums, tables):
    blocks = sums.reshape(sums.shape[0], -1, GROUP + 2, HEAD_DIM)
    turned = rotate(blocks[:, :, : GROUP + 1], tables).astype(jnp.bfloat16)
    return turned, blocks[:, :, GROUP + 1].astype(jnp.bfloat16)


def cache_part(queries, keys_split, values_split, live_count):
    slot_count = keys_split.shape[1]
    scores = jnp.einsum("ngjd,nsgd->ngjs", queries, keys_split, preferred_element_type=jnp.float32) * SCORE_SCALE
    live_mask = (jnp.arange(slot_count, dtype=jnp.int32)[None, :] < live_count[:, None])[:, None, None, :]
    highest = jnp.max(jnp.where(live_mask, scores, -jnp.inf), axis=-1)
    weights = jnp.where(live_mask, jnp.exp(scores - highest[..., None]), 0.0)
    weight_sum = jnp.sum(weights, axis=-1)
    blended = jnp.einsum(
        "ngjs,nsgd->ngjd", weights.astype(jnp.bfloat16), values_split, preferred_element_type=jnp.float32
    )
    return blended, highest, weight_sum


def attend(queries, keys_split, values_split, live_count, fresh):
    blended, highest, weight_sum = cache_part(queries, keys_split, values_split, live_count)
    wide = queries.astype(jnp.float32)
    scores = [
        jnp.sum(wide * key[:, :, None, :].astype(jnp.float32), axis=-1) * SCORE_SCALE for key, _ in fresh
    ]
    joint = highest
    for score in scores:
        joint = jnp.maximum(joint, score)
    share = jnp.exp(highest - joint)
    top = share[..., None] * blended
    bottom = share * weight_sum
    for score, (_, value) in zip(scores, fresh):
        share = jnp.exp(score - joint)
        top = top + share[..., None] * value[:, :, None, :].astype(jnp.float32)
        bottom = bottom + share
    return (top / bottom[..., None]).astype(jnp.bfloat16)


def mix_out(attended, w_out):
    count = lax.axis_size("gx")
    sides = lax.axis_size("gy")
    if not power_of_two(count) or sides != 2 or count % sides:
        partial = jnp.dot(
            lax.all_gather(attended, "gx", axis=0, tiled=True), w_out, preferred_element_type=jnp.float32
        )
        return lax.psum_scatter(partial.astype(jnp.bfloat16), "gy", scatter_dimension=0, tiled=True)
    place = lax.axis_index("gx")
    side = lax.axis_index("gy")
    rows = attended.shape[0]
    held, positions = attended, [0]
    bit = count // 2
    while bit:
        held = jnp.concatenate([held, swap(held, "gx", bit)], axis=0)
        positions = positions + [k ^ bit for k in positions]
        bit //= 2
    spots = jnp.zeros((count,), jnp.int32).at[jnp.array(positions)].set(jnp.arange(count, dtype=jnp.int32))
    share = count // sides

    def half_of(which):
        return jnp.concatenate(
            [
                lax.dynamic_slice_in_dim(held, spots[(which * share + j) ^ place] * rows, rows, 0)
                for j in range(share)
            ],
            axis=0,
        )

    lined = jnp.concatenate([half_of(1 - side), half_of(side)], axis=0)
    partial = jnp.dot(lined, w_out, preferred_element_type=jnp.float32)
    half = partial.shape[0] // 2
    received = swap(partial[:half].astype(jnp.bfloat16), "gy", 1)
    return (partial[half:] + received.astype(jnp.float32)).astype(jnp.bfloat16)


def trade(table, slots, partners):
    count = lax.axis_size("rep")
    replica = lax.axis_index("rep")
    own = table[slots]
    held = [own] + [
        lax.ppermute(own, "rep", [(i, (i + m) % count) for i in range(count)]) for m in range(1, count)
    ]
    away = jnp.mod(replica - partners, count)
    row_ids = jnp.arange(table.shape[0], dtype=jnp.int32)
    for s in range(slots.shape[0]):
        got = held[0][s]
        for m in range(1, count):
            got = jnp.where(away[s] == m, held[m][s], got)
        table = jnp.where((row_ids == slots[s])[:, None], got[None], table)
    return table


def body(hidden_one, hidden_two, w_qkv, w_out, key_cache, value_cache, lengths, mig_rows, dest):
    replica = lax.axis_index("rep")
    replicas = lax.axis_size("rep")
    own_lengths = lengths[replica]
    row_count = own_lengths.shape[0]
    blocks_here = mig_rows.shape[1]
    leave_each = mig_rows.shape[2]
    block_base = jnp.repeat(jnp.arange(blocks_here, dtype=jnp.int32) * ROWS_DEV, leave_each)
    mig_flat = mig_rows.reshape(replicas, -1)
    dest_flat = dest.reshape(replicas, -1)
    leaving = block_base + mig_flat[replica]
    heading = dest_flat[replica]
    replica_ids = jnp.arange(replicas, dtype=jnp.int32)
    came_from = jnp.sum(replica_ids[:, None] * (dest_flat == replica).astype(jnp.int32), axis=0)
    row_ids = jnp.arange(row_count, dtype=jnp.int32)
    from_hit = (row_ids[None, None, :] == (block_base[None] + mig_flat)[:, :, None]) & (
        replica_ids[:, None] == came_from[None]
    )[:, :, None]
    arrive_lengths = jnp.sum(jnp.where(from_hit, lengths[:, None, :], 0), axis=(0, 2))
    land_hit = row_ids[None, :] == leaving[:, None]
    lengths_two = jnp.where(
        jnp.any(land_hit, axis=0), jnp.sum(jnp.where(land_hit, arrive_lengths[:, None], 0), axis=0), own_lengths
    )
    tables_one = turn_tables(own_lengths)
    tables_two = turn_tables(lengths_two + 1)
    keys_split = key_cache.reshape(row_count, key_cache.shape[1], -1, HEAD_DIM)
    values_split = value_cache.reshape(row_count, value_cache.shape[1], -1, HEAD_DIM)
    groups = keys_split.shape[2]

    sums_one = project_sums(gather_rows(hidden_one), w_qkv)
    sums_two = project_sums(gather_rows(hidden_two), w_qkv)

    turned_one, value_one = split_sums(sums_one, tables_one)
    key_one = turned_one[:, :, GROUP]
    fresh_one = (key_one, value_one)
    attended_one = attend(turned_one[:, :, :GROUP], keys_split, values_split, own_lengths, (fresh_one,))
    out_one = mix_out(attended_one.reshape(row_count, -1), w_out)

    turned_two, value_two = split_sums(sums_two, tables_two)
    packed = jnp.concatenate([turned_two, value_two[:, :, None, :]], axis=2).reshape(row_count, -1)
    packed = trade(packed, leaving, heading).reshape(row_count, groups, GROUP + 2, HEAD_DIM)
    fresh_two = (packed[:, :, GROUP], packed[:, :, GROUP + 1])
    attended_two = attend(
        packed[:, :, :GROUP], keys_split, values_split, own_lengths, (fresh_one, fresh_two)
    ).reshape(row_count, -1)
    attended_two = trade(attended_two, leaving, came_from)
    out_two = mix_out(attended_two, w_out)
    return (out_one, out_two)


def solution(mesh):
    placed = (
        P(("rep", "gy"), "gx"),
        P(("rep", "gy"), "gx"),
        P("gx", "gy"),
        P("gy", "gx"),
        P(("rep", "gx"), None, "gy"),
        P(("rep", "gx"), None, "gy"),
        P(None, "gx"),
        P(None, "gx", None),
        P(None, "gx", None),
    )
    return jax.shard_map(
        body,
        mesh=mesh,
        in_specs=placed,
        out_specs=(P(("rep", "gy"), "gx"), P(("rep", "gy"), "gx")),
        check_vma=False,
    )
```

```python
import math

import jax
import jax.numpy as jnp
from jax import lax
from jax.experimental import pallas as pl
from jax.experimental.pallas import tpu as pltpu
from jax.sharding import PartitionSpec as P


HEADS = 64
KV_HEADS = 8
HEAD_DIM = 128
ROWS_DEV = 16
GROUP = HEADS // KV_HEADS
ROPE_BASE = 500000.0
LINK_SCALE = 16.0
STEP = 16
CHUNKS = 2
SCORE_SCALE = 1.0 / math.sqrt(HEAD_DIM)


def swap(value, axis, bit):
    count = lax.axis_size(axis)
    return lax.ppermute(value, axis, [(i, i ^ bit) for i in range(count)])


def power_of_two(count):
    return count & (count - 1) == 0


def gather_rows(hidden, after=None):
    if lax.axis_size("gy") != 2:
        return lax.all_gather(hidden, "gy", axis=0, tiled=True)
    peer = swap(hidden, "gy", 1)
    if after is not None:
        peer, _ = lax.optimization_barrier((peer, after))
    first = lax.axis_index("gy") == 0
    return jnp.concatenate([jnp.where(first, hidden, peer), jnp.where(first, peer, hidden)], axis=0)


def narrow(value):
    return (value * LINK_SCALE).astype(jnp.float16)


def widen(value):
    return value.astype(jnp.float32) * (1.0 / LINK_SCALE)


def line_up(gathered):
    count = lax.axis_size("gx")
    if not power_of_two(count):
        return gathered
    place = lax.axis_index("gx")
    rows = gathered.shape[0] // count
    order = sorted(range(count), key=lambda k: [1 - (k >> b & 1) for b in range(count.bit_length() - 1)])
    blocks = [lax.dynamic_slice_in_dim(gathered, (place ^ k) * rows, rows, 0) for k in order]
    return jnp.concatenate(blocks, axis=0)


def project_sums(lined, w_qkv, chunks, after=None):
    count = lax.axis_size("gx")
    width = w_qkv.shape[1] // chunks
    parts = []
    for c in range(chunks):
        weights = w_qkv[:, c * width : (c + 1) * width]
        parts.append(jnp.dot(lined, weights, preferred_element_type=jnp.float32))
    if not power_of_two(count):
        parts = [lax.psum_scatter(part, "gx", scatter_dimension=0, tiled=True) for part in parts]
    sent = parts[0][:1, :1]
    bit = 1
    while bit < count and power_of_two(count):
        half = parts[0].shape[0] // 2
        for c in range(chunks):
            sent = narrow(parts[c][:half])
            received = swap(sent, "gx", bit)
            if after is not None:
                received, _ = lax.optimization_barrier((received, after))
            parts[c] = parts[c][half:] + widen(received)
        bit *= 2
    return parts, sent


def turn_tables(positions):
    half_dim = HEAD_DIM // 2
    inverse = ROPE_BASE ** (-(jnp.arange(half_dim, dtype=jnp.float32) * 2.0 / HEAD_DIM))
    angles = positions.astype(jnp.float32)[:, None] * inverse
    cosine, sine = jnp.cos(angles), jnp.sin(angles)
    return jnp.concatenate([cosine, cosine], axis=-1), jnp.concatenate([-sine, sine], axis=-1)


def attend_block(lengths, sums, cosine, sine, *rest):
    *earlier, keys, values, attended, fresh, turned, merged = rest
    groups = keys.shape[2] // HEAD_DIM
    heads = groups * GROUP
    each = GROUP + 2
    steps = sums.shape[0]
    first = pl.program_id(0) * steps
    slot_ids = lax.broadcasted_iota(jnp.int32, (heads, keys.shape[1]), 1)
    head_group = lax.broadcasted_iota(jnp.int32, (heads, HEAD_DIM), 0) // GROUP

    def lanes(at):
        return slice(at * HEAD_DIM, (at + 1) * HEAD_DIM)

    def stack(per_row):
        return jnp.concatenate([per_row(r) for r in range(steps)], axis=0)

    def over_heads(table, base):
        return stack(
            lambda r: jnp.concatenate(
                [jnp.broadcast_to(table[r : r + 1, lanes(2 * g + base)], (GROUP, HEAD_DIM)) for g in range(groups)],
                axis=0,
            )
        )

    for at in range(groups * each):
        block = sums[:, lanes(at)]
        if at % each <= GROUP:
            block = block * cosine[...] + pltpu.roll(block, HEAD_DIM // 2, 1) * sine[...]
        block = block.astype(jnp.bfloat16).astype(jnp.float32)
        if at % each < GROUP:
            turned[pl.ds(at // each * GROUP + at % each, steps, stride=heads), :] = block
        else:
            fresh[:, lanes(at // each * 2 + at % each - GROUP)] = block
    query = turned[...]

    def row_scores(r):
        mine = query[r * heads : (r + 1) * heads]
        spread = jnp.concatenate([jnp.where(head_group == g, mine, 0.0) for g in range(groups)], axis=1)
        raw = lax.dot_general(
            spread.astype(jnp.bfloat16), keys[r], (((1,), (1,)), ((), ())), preferred_element_type=jnp.float32
        )
        return jnp.where(slot_ids < lengths[first + r], raw * SCORE_SCALE, -jnp.inf)

    def row_blend(r):
        whole = jnp.dot(
            weights[r * heads : (r + 1) * heads].astype(jnp.bfloat16), values[r],
            preferred_element_type=jnp.float32,
        )
        return jnp.concatenate(
            [whole[g * GROUP : (g + 1) * GROUP, g * HEAD_DIM : (g + 1) * HEAD_DIM] for g in range(groups)], axis=0
        )

    scores = stack(row_scores)
    highest = jnp.max(scores, axis=1, keepdims=True)
    weights = jnp.exp(scores - highest)
    weight_sum = jnp.sum(weights, axis=1, keepdims=True)
    blended = stack(row_blend)
    sources = list(earlier) + [fresh]
    marks = [
        jnp.sum(query * over_heads(e, 0), axis=1, keepdims=True) * SCORE_SCALE for e in sources
    ]
    joint = highest
    for mark in marks:
        joint = jnp.maximum(joint, mark)
    share = jnp.exp(highest - joint)
    top, bottom = share * blended, share * weight_sum
    for mark, e in zip(marks, sources):
        share = jnp.exp(mark - joint)
        top = top + share * over_heads(e, 1)
        bottom = bottom + share
    merged[...] = top / bottom
    for h in range(heads):
        attended[:, lanes(h)] = merged[pl.ds(h, steps, stride=heads), :].astype(jnp.bfloat16)


def attend(sums, tables, earlier, key_cache, value_cache, lengths, chunk, chunks):
    row_count, slots, width = key_cache.shape
    width = width // chunks
    groups = width // HEAD_DIM
    step = next(n for n in (STEP, 8, 1) if row_count % n == 0)

    def rows(*shape):
        return pl.BlockSpec((step,) + shape, lambda i, _: (i,) + (0,) * len(shape))

    heads = groups * GROUP
    fresh = rows(2 * width)
    before = pl.BlockSpec((step, 2 * width), lambda i, _: (i, chunk))
    cache = pl.BlockSpec((step, slots, width), lambda i, _: (i, 0, chunk))
    return pl.pallas_call(
        attend_block,
        grid_spec=pltpu.PrefetchScalarGridSpec(
            num_scalar_prefetch=1,
            grid=(row_count // step,),
            in_specs=[rows(sums.shape[1]), rows(HEAD_DIM), rows(HEAD_DIM)]
            + [before for _ in earlier]
            + [cache, cache],
            out_specs=[rows(heads * HEAD_DIM), fresh],
            scratch_shapes=[pltpu.VMEM((step * heads, HEAD_DIM), jnp.float32) for _ in range(2)],
        ),
        out_shape=[
            jax.ShapeDtypeStruct((row_count, heads * HEAD_DIM), jnp.bfloat16),
            jax.ShapeDtypeStruct((row_count, 2 * width), jnp.float32),
        ],
        compiler_params=pltpu.CompilerParams(vmem_limit_bytes=16 * 1024 * 1024),
        cost_estimate=pl.CostEstimate(
            flops=8 * row_count * heads * slots * width,
            bytes_accessed=4 * row_count * slots * width,
            transcendentals=0,
        ),
    )(lengths, sums, *tables, *earlier, key_cache, value_cache)


def reverse_bits(value, count):
    turned = value * 0
    bit = count // 2
    while bit:
        turned = turned + (value & 1) * bit
        value = value >> 1
        bit //= 2
    return turned


def spread_rows(own, extra=None):
    held = own
    bit = lax.axis_size("gx") // 2
    while bit:
        sent = held if extra is None or bit > 1 else jnp.concatenate([held, extra], axis=0)
        other = swap(sent, "gx", bit)
        if extra is not None and bit == 1:
            extra = jnp.concatenate([extra, other[held.shape[0] :]], axis=0)
            other = other[: held.shape[0]]
        held = jnp.concatenate([held, other], axis=0)
        bit //= 2
    return held if extra is None else (held, extra)


def by_side(held, rows):
    count = lax.axis_size("gx")
    place, side = lax.axis_index("gx"), lax.axis_index("gy")
    share = count // 2
    spots = [(1 - side) * share + j for j in range(share)] + [side * share + j for j in range(share)]
    return jnp.concatenate(
        [lax.dynamic_slice_in_dim(held, reverse_bits(c ^ place, count) * rows, rows, 0) for c in spots], axis=0
    )


def pairwise():
    count = lax.axis_size("gx")
    return power_of_two(count) and count > 1 and lax.axis_size("gy") == 2


def mix_rows(attended, w_out):
    partial = jnp.dot(
        lax.all_gather(attended, "gx", axis=0, tiled=True), w_out, preferred_element_type=jnp.float32
    )
    return lax.psum_scatter(partial.astype(jnp.bfloat16), "gy", scatter_dimension=0, tiled=True)


def mix_lined(lined, w_out):
    partial, start = None, 0
    for part in lined:
        weights = w_out[start : start + part.shape[1]]
        piece = jnp.dot(part, weights, preferred_element_type=jnp.float32)
        partial = piece if partial is None else partial + piece
        start += part.shape[1]
    half = partial.shape[0] // 2
    received = swap(partial[:half].astype(jnp.bfloat16), "gy", 1)
    return (partial[half:] + received.astype(jnp.float32)).astype(jnp.bfloat16)


def pick_rows(hits, rows):
    return jnp.dot(hits.astype(jnp.bfloat16), rows, preferred_element_type=jnp.float32).astype(jnp.bfloat16)


def all_replicas(own):
    count = lax.axis_size("rep")
    held = [own]
    for m in range(1, count):
        held.append(lax.ppermute(own, "rep", [(i, (i + m) % count) for i in range(count)]))
    return jnp.concatenate(held, axis=0)


def partner_hits(partners):
    count = lax.axis_size("rep")
    slots = partners.shape[0]
    away = jnp.mod(lax.axis_index("rep") - partners, count)
    columns = jnp.arange(count * slots, dtype=jnp.int32)
    return (away * slots + jnp.arange(slots, dtype=jnp.int32))[:, None] == columns[None, :]


def row_hits(row_count, slots):
    return jnp.arange(row_count, dtype=jnp.int32)[:, None] == slots[None, :]


def replace_rows(table, hits, rows):
    return jnp.where(jnp.any(hits, axis=1)[:, None], pick_rows(hits, rows), table)


def table_of_all(local):
    count = lax.axis_size("gx")
    if not power_of_two(count):
        return lax.all_gather(local, "gx", axis=2, tiled=True)
    here = (jnp.arange(count, dtype=jnp.int32) == lax.axis_index("gx"))[None, None, :, None, None]
    full = jnp.where(here, local[:, :, None], 0)
    bit = 1
    while bit < count:
        other = swap(full, "gx", bit)
        full = full + other
        bit *= 2
    return full.reshape(local.shape[0], local.shape[1], -1, local.shape[3])


def own_slots(mig, dest):
    replica = lax.axis_index("rep")
    base = (jnp.arange(mig.shape[1], dtype=jnp.int32) * ROWS_DEV)[:, None]
    leaving = (base + mig[replica]).reshape(-1)
    heading = dest[replica].reshape(-1)
    ids = jnp.arange(mig.shape[0], dtype=jnp.int32)[:, None, None]
    came_from = jnp.sum(jnp.where(dest == replica, ids, 0), axis=0).reshape(-1)
    return leaving, heading, came_from


def steps(hidden_one, hidden_two, w_qkv, w_out, key_cache, value_cache, lengths, mig_rows, dest):
    replica = lax.axis_index("rep")
    own_lengths = lengths[replica]
    row_count = own_lengths.shape[0]
    tables = table_of_all(jnp.stack([mig_rows, dest]))
    side_blocks = tables.shape[2] // lax.axis_size("gy")
    ours = lax.dynamic_slice_in_dim(tables, lax.axis_index("gy") * side_blocks, side_blocks, 2)

    all_leaving, _, _ = own_slots(tables[0], tables[1])

    lined_one = line_up(gather_rows(hidden_one))
    gathered_two = gather_rows(hidden_two, lined_one)
    side_leaving, side_heading, _ = own_slots(ours[0], ours[1])
    side_hits = row_hits(hidden_two.shape[0], side_leaving)
    moved = pick_rows(partner_hits(side_heading), all_replicas(pick_rows(side_hits.T, hidden_two)))
    moved = gather_rows(moved, lined_one)
    gathered_two = replace_rows(gathered_two, row_hits(gathered_two.shape[0], all_leaving), moved)

    groups = key_cache.shape[2] // HEAD_DIM
    chunks = next(n for n in (CHUNKS, 1) if groups % n == 0)
    (sums_one,), last_sent = project_sums(lined_one, w_qkv, 1)
    sums_two, _ = project_sums(line_up(gathered_two), w_qkv, chunks, last_sent)
    attended_one, new_one = attend(sums_one, turn_tables(own_lengths), (), key_cache, value_cache, own_lengths, 0, 1)
    tables_two = turn_tables(own_lengths + 1)
    attended_two = [
        attend(part, tables_two, (new_one,), key_cache, value_cache, own_lengths, c, chunks)[0]
        for c, part in enumerate(sums_two)
    ]

    leaving, _, came_from = own_slots(mig_rows, dest)
    leave_hits = row_hits(row_count, leaving)
    sent = jnp.concatenate([pick_rows(leave_hits.T, part) for part in attended_two], axis=1)
    returned = pick_rows(partner_hits(came_from), all_replicas(sent))
    if not pairwise():
        table = replace_rows(jnp.concatenate(attended_two, axis=1), leave_hits, returned)
        return (mix_rows(attended_one, w_out), mix_rows(table, w_out))
    out_one = mix_lined([by_side(spread_rows(attended_one), row_count)], w_out)
    slots, width = returned.shape[0], attended_two[0].shape[1]
    held, bit = returned, lax.axis_size("gx") // 2
    while bit > 1:
        held = jnp.concatenate([held, swap(held, "gx", bit)], axis=0)
        bit //= 2
    extra = jnp.concatenate([held[:, c * width : (c + 1) * width] for c in range(chunks)], axis=0)
    lined = [spread_rows(part) for part in attended_two[:-1]]
    last, extra = spread_rows(attended_two[-1], extra)
    lined = [by_side(part, row_count) for part in lined + [last]]
    extra = extra.reshape(2, chunks, held.shape[0], width)
    fixed = [by_side(extra[:, c].reshape(-1, width), slots) for c in range(chunks)]
    half_slots, half_rows = all_leaving.shape[0] // 2, lined[0].shape[0] // 2
    lined_slots = jnp.where(
        lax.axis_index("gy") == 0,
        jnp.concatenate([all_leaving[half_slots:] - half_rows, all_leaving[:half_slots] + half_rows]),
        all_leaving,
    )
    hits = row_hits(2 * half_rows, lined_slots)
    lined = [lax.optimization_barrier(replace_rows(part, hits, rows)) for part, rows in zip(lined, fixed)]
    return (out_one, mix_lined(lined, w_out))


def solution(mesh):
    placed = (
        P(("rep", "gy"), "gx"),
        P(("rep", "gy"), "gx"),
        P("gx", "gy"),
        P("gy", "gx"),
        P(("rep", "gx"), None, "gy"),
        P(("rep", "gx"), None, "gy"),
        P(None, "gx"),
        P(None, "gx", None),
        P(None, "gx", None),
    )
    return jax.shard_map(
        steps,
        mesh=mesh,
        in_specs=placed,
        out_specs=(P(("rep", "gy"), "gx"), P(("rep", "gy"), "gx")),
        check_vma=False,
    )
```
